256 devices in a mesh: inst: 4 (over y_hi, core), cells: 64 (over y_lo, x, z).
Axes of the slice: x: 4, y: 4 (y_hi: 2, y_lo: 2; y = y_hi * 2 + y_lo), z: 8, core: 2. Of those that a mesh axis runs over, the one named last changes fastest.
Arguments:
- flow_state: float32 [8, 5, 512, 32, 128], P('inst', None, 'cells'), may hold values from -6 to 6
- forcing: float32 [8, 5, 512, 32, 128], P('inst', None, 'cells'), may hold values from -6 to 6
- diffusion: float32 [512, 32, 128], P('cells'), may hold values from 0.2 to 0.6
- block_inverse: float32 [5, 5, 512, 32, 128], P(None, None, 'cells', 'inst'), may hold values from -0.03 to 0.15, as said below
Outputs:
- new_state: float32 [8, 5, 512, 32, 128], P('inst', None, 'cells')
The draws below stay inside these ranges and needn't reach their ends.
Inputs may be any that keep to these rules, and one draw needn't show every extreme that they name: block_inverse[v, v] lies between 0.06 and 0.15; entries off the diagonal lie between -0.03 and 0.03.
All inputs are finite; a program needn't handle non-finite values.
Results may differ from the reference program's by a relative error of at most 0.0001.
Values sent between devices are 32-bit elements; how exact they have to be, the bound alone decides.
A program may use at most 64 MiB of HBM per device.

```python
import math
import jax
import jax.numpy as jnp
from jax import lax

INSTANCES = 8
VARIABLES = 5
NZ = 128
SWEEPS = 4
NX = 512
NY = 32


def draw_block_inverse(key, part):
    first_key, second_key = jax.random.split(jax.random.fold_in(key, 17))
    shape = (VARIABLES, VARIABLES, NX, NY, NZ)
    diagonal_vals = 0.06 * jnp.exp(jax.random.uniform(first_key, shape) * math.log(2.5))
    off_vals = jnp.clip(0.012 * jax.random.normal(second_key, shape), -0.03, 0.03)
    identity = jnp.eye(VARIABLES)[:, :, None, None, None]
    return jnp.where(identity > 0.5, diagonal_vals, off_vals).astype(jnp.float32)


def block_levels(key, shape, cuts, smallest, top_value):
    def one(dim, parts):
        steps = jax.random.uniform(jax.random.fold_in(jax.random.fold_in(key, 6), dim), (parts,), jnp.float32, smallest / len(cuts), top_value / len(cuts))
        return jnp.repeat(jnp.exp(steps), shape[dim] // parts).reshape((-1,) + (1,) * (len(shape) - dim - 1))

    loudness = one(*cuts[0])
    for cut in cuts[1:]:
        loudness = loudness * one(*cut)
    return loudness


def noise(own_key, dims, spread, most, cuts=(), held_as=jnp.bfloat16):
    values = jax.random.normal(own_key, dims, jnp.float32) * spread
    if len(cuts) > 0:
        values = block_levels(own_key, dims, cuts, -0.22, 0.18) * values
    return jnp.clip(values, min=-most, max=most).astype(held_as)


def setup_inputs(seed: int = 0) -> dict:
    arg_keys = jax.random.split(jax.random.key(seed), 5)
    return {
        "flow_state": noise(arg_keys[0], (INSTANCES, VARIABLES, NX, NY, NZ), 1.0, 6.0, ((0, 4), (2, 64)), jnp.float32),
        "forcing": noise(arg_keys[1], (INSTANCES, VARIABLES, NX, NY, NZ), 1.0, 6.0, ((0, 4), (2, 64)), jnp.float32),
        "diffusion": jnp.clip(jnp.exp(math.log(0.6) - 1.0986123 * jax.random.uniform(arg_keys[2], (NX, NY, NZ), jnp.float32) ** block_levels(arg_keys[2], (NX, NY, NZ), ((0, 64),), -0.2, 0.2)), 0.2, 0.6),
        "block_inverse": draw_block_inverse(jax.random.fold_in(arg_keys[4], 71), 0),
    }


frequency = 1.0


def spectral_matrix(count):
    index = jnp.arange(count)
    offset = index[:, None] - index[None, :]
    parity = jnp.where(offset % 2 == 0, 1.0, -1.0)
    angle = math.pi * jnp.where(offset == 0, 1, offset) / count
    entries = 0.5 * parity / jnp.tan(angle)
    return jnp.where(offset == 0, 0.0, entries).astype(jnp.float32)


def neighbour_sum(grid_field):
    padded = jnp.pad(grid_field, ((0, 0), (0, 0), (1, 1), (1, 1), (1, 1)))
    beside = padded[:, :, 2:, 1:-1, 1:-1] + padded[:, :, :-2, 1:-1, 1:-1]
    beside = beside + padded[:, :, 1:-1, 2:, 1:-1] + padded[:, :, 1:-1, :-2, 1:-1]
    beside = beside + padded[:, :, 1:-1, 1:-1, 2:] + padded[:, :, 1:-1, 1:-1, :-2]
    return beside


def spectral_term(matrix, grid_field):
    flat = grid_field.reshape(grid_field.shape[0], -1)
    product = jnp.dot(matrix, flat, precision=lax.Precision.HIGHEST)
    return (frequency * product).reshape(grid_field.shape)


def apply_blocks(block_inverse, source):
    return jnp.einsum("vwxyz,nwxyz->nvxyz", block_inverse, source, precision=lax.Precision.HIGHEST)


def reference(flow_state, forcing, diffusion, block_inverse):
    matrix = spectral_matrix(INSTANCES)
    weight = diffusion[None, None]
    residual = weight * (6.0 * flow_state - neighbour_sum(flow_state)) - forcing + spectral_term(matrix, flow_state)
    update = apply_blocks(block_inverse, -residual)
    for sweep_index in range(SWEEPS):
        source = -residual - spectral_term(matrix, update) + weight * neighbour_sum(update)
        update = apply_blocks(block_inverse, source)
    return flow_state + update
```

```python
import functools
import math

import jax
import jax.numpy as jnp
from jax import lax
from jax.experimental import pallas as pl
from jax.experimental.pallas import tpu as pltpu
from jax.sharding import PartitionSpec as P

SWEEPS = 4
HALF = math.sqrt(0.5)
MESH = pl.DeviceIdType.MESH


def to_modes(x):
    e = [x[n] + x[n + 4] for n in range(4)]
    o = [x[n] - x[n + 4] for n in range(4)]
    even, odd = e[0] + e[2], e[1] + e[3]
    minus, plus = HALF * (o[1] - o[3]), HALF * (o[1] + o[3])
    return [even + odd, even - odd, o[0] + minus, plus + o[2], e[0] - e[2], e[1] - e[3], o[0] - minus, plus - o[2]]


def from_modes(a):
    even, odd = 0.125 * (a[0] + a[1]), 0.125 * (a[0] - a[1])
    c2, s2 = 0.25 * a[4], 0.25 * a[5]
    e = [even + c2, odd + s2, even - c2, odd - s2]
    c, s = a[2] - a[6], a[3] + a[7]
    o = [0.25 * (a[2] + a[6]), (0.25 * HALF) * (s + c), 0.25 * (a[3] - a[7]), (0.25 * HALF) * (s - c)]
    return [e[n] + o[n] for n in range(4)] + [e[n] - o[n] for n in range(4)]


def kernel(cells, fs_hbm, forcing_hbm, diff_hbm, block_hbm, out_hbm,
           fs, forcing, diff, block, halo, local, fm, rm, neg, u, edge_out, edge_in, back, out,
           load_sem, own_sem, halo_s, halo_r, fs_s, fs_r, part_s, part_r, x_s, x_r, y_s, y_r, back_s, back_r, out_sem):
    i, k = lax.axis_index("inst"), lax.axis_index("cells")
    peers = (i + 1 - 2 * lax.rem(i, 2), lax.rem(i + 2, 4), 3 - i)
    has_left, has_right = k > 0, k < cells - 1
    has_up, has_down = i > 0, i < 3
    own_rows = pl.ds(pl.multiple_of(8 * i, 8), 8)

    loads = [
        pltpu.make_async_copy(fs_hbm, fs, load_sem.at[0]),
        pltpu.make_async_copy(forcing_hbm, forcing, load_sem.at[1]),
        pltpu.make_async_copy(diff_hbm, diff, load_sem.at[2]),
        pltpu.make_async_copy(block_hbm, block, load_sem.at[3]),
        pltpu.make_async_copy(fs_hbm.at[:, :, :, own_rows, :], fm.at[pl.ds(2 * i, 2)], own_sem),
    ]
    for load in loads:
        load.start()

    barrier = pltpu.get_barrier_semaphore()
    for peer in peers:
        pl.semaphore_signal(barrier, inc=1, device_id=(peer, k), device_id_type=MESH)

    @pl.when(has_left)
    def _():
        pl.semaphore_signal(barrier, inc=1, device_id=(i, k - 1), device_id_type=MESH)

    @pl.when(has_right)
    def _():
        pl.semaphore_signal(barrier, inc=1, device_id=(i, k + 1), device_id_type=MESH)

    pl.semaphore_wait(barrier, 3 + has_left.astype(jnp.int32) + has_right.astype(jnp.int32))

    def remote(src, dst, send, recv, device):
        return pltpu.make_async_remote_copy(
            src_ref=src, dst_ref=dst, send_sem=send, recv_sem=recv, device_id=device, device_id_type=MESH)

    def rows_of(peer):
        return pl.ds(pl.multiple_of(8 * peer, 8), 8)

    def fs_copy(x, slot):
        peer = peers[slot]
        return remote(fs.at[:, :, x, rows_of(peer), :], fm.at[pl.ds(2 * i, 2), :, x],
                      fs_s.at[x, slot], fs_r.at[x, slot], (peer, k))

    def part_copy(x, slot):
        peer = peers[slot]
        return remote(local.at[:, :, x, rows_of(peer), :], rm.at[pl.ds(2 * i, 2), :, x],
                      part_s.at[x, slot], part_r.at[x, slot], (peer, k))

    def back_copy(x, slot):
        peer = peers[slot]
        return remote(back.at[peer, x], out.at[:, :, x, own_rows, :],
                      back_s.at[x, slot], back_r.at[x, slot], (peer, k))

    def pair(p):
        return (p, 7 - p)

    def send(copy, p):
        for slot in (1, 2, 0):
            for x in pair(p):
                copy(x, slot).start()

    def arrived(copy, p):
        for slot in range(3):
            for x in pair(p):
                copy(x, slot).wait_recv()

    def fs_edge(side):
        return remote(fs.at[:, :, 7 if side else 0], halo.at[1 - side], halo_s.at[side], halo_r.at[1 - side],
                      (i, k + (1 if side else -1)))

    def x_edge(s, side):
        return remote(u.at[s, 8 if side else 1], u.at[s, 0 if side else 9], x_s.at[s, side], x_r.at[s, 1 - side],
                      (i, k + (1 if side else -1)))

    def y_edge(s, p, side):
        return remote(edge_out.at[s, side, p], edge_in.at[s, 1 - side, p], y_s.at[s, side, p], y_r.at[s, 1 - side, p],
                      (i + (1 if side else -1), k))

    def both(first, second, action):
        pl.when(first)(lambda: action(0))
        pl.when(second)(lambda: action(1))

    loads[0].wait()
    both(has_left, has_right, lambda side: fs_edge(side).start())
    send(fs_copy, 0)
    send(fs_copy, 1)

    def clear(ref, lead):
        zeros = jnp.zeros((8, 128), jnp.float32)

        def body(t, carry):
            ref[(*lead, pl.ds(pl.multiple_of(8 * t, 8), 8), slice(None))] = zeros
            return carry

        lax.fori_loop(0, ref.shape[-2] // 8, body, 0)

    def clear_x(side):
        for n in range(2):
            for v in range(5):
                clear(halo, (side, n, v))
        for s in range(SWEEPS):
            clear(u, (s, 9 if side else 0))

    def clear_y(side):
        for s in range(SWEEPS):
            for p in range(4):
                for t in range(2):
                    clear(edge_in, (s, side, p, t))

    both(jnp.logical_not(has_left), jnp.logical_not(has_right), clear_x)
    both(jnp.logical_not(has_up), jnp.logical_not(has_down), clear_y)

    loads[1].wait()
    loads[2].wait()

    def shifted_sum(c, low, high):
        n = c.shape[0]
        row = lax.broadcasted_iota(jnp.int32, c.shape, 0)
        lane = lax.broadcasted_iota(jnp.int32, c.shape, 1)
        up = jnp.where(row == 0, low, pltpu.roll(c, 1, 0))
        down = jnp.where(row == n - 1, high, pltpu.roll(c, n - 1, 0))
        left = jnp.where(lane == 0, 0.0, pltpu.roll(c, 1, 1))
        right = jnp.where(lane == 127, 0.0, pltpu.roll(c, 127, 1))
        return (up + down) + (left + right)

    def local_plane(x, before, after):
        weight = diff[x]
        for n in range(2):
            for v in range(5):
                c = fs[n, v, x]
                beside = shifted_sum(c, 0.0, 0.0) + (before(n, v) + after(n, v))
                local[n, v, x] = weight * (6.0 * c - beside) - forcing[n, v, x]
        for n in range(2):
            for v in range(5):
                rm[2 * i + n, v, x] = local[n, v, x, own_rows, :]

    def inner(x, carry):
        local_plane(x, lambda n, v: fs[n, v, x - 1], lambda n, v: fs[n, v, x + 1])
        return carry

    lax.fori_loop(1, 7, inner, 0)

    def fs_edge_arrived(side):
        remote(halo.at[side], halo.at[side], halo_s.at[side], halo_r.at[side], (i, k)).wait_recv()

    both(has_left, has_right, fs_edge_arrived)
    local_plane(0, lambda n, v: halo[0, n, v], lambda n, v: fs[n, v, 1])
    local_plane(7, lambda n, v: fs[n, v, 6], lambda n, v: halo[1, n, v])
    send(part_copy, 0)
    send(fs_copy, 2)
    loads[3].wait()
    loads[4].wait()

    def tile(m, v):
        return pl.ds((m * 5 + v) * 8, 8)

    def plane_of(p, t):
        return p + t * (7 - 2 * p)

    def store_edges(s, p, t, x):
        edge_out[s, 0, p, t] = u[s, x + 1, pl.ds(0, 40, stride=8), :]
        edge_out[s, 1, p, t] = u[s, x + 1, pl.ds(7, 40, stride=8), :]

    def apply_block(s, x, m, source):
        for v in range(5):
            total = block[v, 0, x] * source[0]
            for w in range(1, 5):
                total = total + block[v, w, x] * source[w]
            u[s, x + 1, tile(m, v), :] = total

    def first_plane(x):
        for v in range(5):
            f = to_modes([fm[n, v, x] for n in range(8)])
            r = to_modes([rm[n, v, x] for n in range(8)])
            neg[x, tile(0, v), :] = -r[0]
            neg[x, tile(1, v), :] = -r[1]
            for q in range(1, 4):
                neg[x, tile(2 * q, v), :] = -(r[2 * q] + q * f[2 * q + 1])
                neg[x, tile(2 * q + 1, v), :] = q * f[2 * q] - r[2 * q + 1]
        for m in range(8):
            apply_block(0, x, m, [neg[x, tile(m, v), :] for v in range(5)])

    def sweep_plane(s, p, t):
        x = plane_of(p, t)
        weight = diff[x, own_rows, :]
        for q in range(4):
            c = [[u[s - 1, x + 1, tile(2 * q + j, v), :] for v in range(5)] for j in range(2)]
            for j in range(2):
                source = []
                for v in range(5):
                    here = tile(2 * q + j, v)
                    at = (2 * q + j) * 5 + v
                    beside = shifted_sum(c[j][v], edge_in[s - 1, 0, p, t, pl.ds(at, 1), :],
                                         edge_in[s - 1, 1, p, t, pl.ds(at, 1), :])
                    beside = beside + (u[s - 1, x, here, :] + u[s - 1, x + 2, here, :])
                    value = weight * beside + neg[x, here, :]
                    if q:
                        value = value + (float(q) * c[0][v] if j else float(-q) * c[1][v])
                    source.append(value)
                apply_block(s, x, 2 * q + j, source)

    def back_plane(x):
        for v in range(5):
            modes = from_modes([u[SWEEPS, x + 1, tile(m, v), :] for m in range(8)])
            for n in range(8):
                back[n // 2, x, n % 2, v] = fm[n, v, x] + modes[n]
        for n in range(2):
            for v in range(5):
                out[n, v, x, own_rows, :] = back[i, x, n, v]

    def y_arrived(s, p):
        def wait(side):
            remote(edge_in.at[s, side, p], edge_in.at[s, side, p], y_s.at[s, side, p], y_r.at[s, side, p], (i, k)).wait_recv()
        both(has_up, has_down, wait)

    def x_arrived(s):
        def wait(side):
            place = u.at[s, 9 if side else 0]
            remote(place, place, x_s.at[s, side], x_r.at[s, side], (i, k)).wait_recv()
        both(has_left, has_right, wait)

    for d in range(8):
        if d < 4:
            arrived(fs_copy, d)
            arrived(part_copy, d)

            def first(t, carry, d=d):
                x = plane_of(d, t)
                first_plane(x)
                store_edges(0, d, t, x)
                return carry

            lax.fori_loop(0, 2, first, 0)
            both(has_up, has_down, lambda side: y_edge(0, d, side).start())
            if d == 0:
                both(has_left, has_right, lambda side: x_edge(0, side).start())
        for s in range(max(1, d - 3), min(4, d) + 1):
            p = d - s
            y_arrived(s - 1, p)
            if p == 0:
                x_arrived(s - 1)

            def sweep(t, carry, s=s, p=p):
                sweep_plane(s, p, t)
                if s < SWEEPS:
                    store_edges(s, p, t, plane_of(p, t))
                else:
                    back_plane(plane_of(p, t))
                return carry

            lax.fori_loop(0, 2, sweep, 0)
            if s < SWEEPS:
                both(has_up, has_down, lambda side: y_edge(s, p, side).start())
                if p == 0:
                    both(has_left, has_right, lambda side: x_edge(s, side).start())
            else:
                send(back_copy, p)
        if d == 0:
            send(part_copy, 1)
            send(fs_copy, 3)
        if d == 1:
            send(part_copy, 2)
            send(part_copy, 3)

    writes = []
    for p in range(4):
        arrived(back_copy, p)
        for x in pair(p):
            write = pltpu.make_async_copy(out.at[:, :, x], out_hbm.at[:, :, x], out_sem.at[x])
            write.start()
            writes.append(write)

    both(has_left, has_right, lambda side: fs_edge(side).wait_send())
    for s in range(SWEEPS):
        both(has_left, has_right, lambda side: x_edge(s, side).wait_send())
        for p in range(4):
            both(has_up, has_down, lambda side: y_edge(s, p, side).wait_send())
    for copy in (fs_copy, part_copy, back_copy):
        for x in range(8):
            for slot in range(3):
                copy(x, slot).wait_send()
    for write in writes:
        write.wait()


def on_device(cells, flow_state, forcing, diffusion, block_inverse):
    f32 = jnp.float32
    dma = pltpu.SemaphoreType.DMA
    any_spec = pl.BlockSpec(memory_space=pl.ANY)
    return pl.pallas_call(
        functools.partial(kernel, cells),
        out_shape=jax.ShapeDtypeStruct(flow_state.shape, f32),
        in_specs=[any_spec] * 4,
        out_specs=any_spec,
        scratch_shapes=[
            pltpu.VMEM((2, 5, 8, 32, 128), f32),
            pltpu.VMEM((2, 5, 8, 32, 128), f32),
            pltpu.VMEM((8, 32, 128), f32),
            pltpu.VMEM((5, 5, 8, 8, 128), f32),
            pltpu.VMEM((2, 2, 5, 32, 128), f32),
            pltpu.VMEM((2, 5, 8, 32, 128), f32),
            pltpu.VMEM((8, 5, 8, 8, 128), f32),
            pltpu.VMEM((8, 5, 8, 8, 128), f32),
            pltpu.VMEM((8, 320, 128), f32),
            pltpu.VMEM((SWEEPS + 1, 10, 320, 128), f32),
            pltpu.VMEM((SWEEPS, 2, 4, 2, 40, 128), f32),
            pltpu.VMEM((SWEEPS, 2, 4, 2, 40, 128), f32),
            pltpu.VMEM((4, 8, 2, 5, 8, 128), f32),
            pltpu.VMEM((2, 5, 8, 32, 128), f32),
            dma((4,)),
            dma(()),
            dma((2,)), dma((2,)),
            dma((8, 3)), dma((8, 3)),
            dma((8, 3)), dma((8, 3)),
            dma((SWEEPS, 2)), dma((SWEEPS, 2)),
            dma((SWEEPS, 2, 4)), dma((SWEEPS, 2, 4)),
            dma((8, 3)), dma((8, 3)),
            dma((8,)),
        ],
        compiler_params=pltpu.CompilerParams(
            collective_id=0, has_side_effects=True, vmem_limit_bytes=56 * 1024 * 1024),
        name="update",
    )(flow_state, forcing, diffusion, block_inverse)


def solution(mesh):
    in_specs = (
        P("inst", None, "cells", None, None),
        P("inst", None, "cells", None, None),
        P("cells", None, None),
        P(None, None, "cells", "inst", None),
    )
    out_specs = P("inst", None, "cells", None, None)
    return jax.shard_map(
        functools.partial(on_device, mesh.shape["cells"]),
        mesh=mesh, in_specs=in_specs, out_specs=out_specs, check_vma=False,
    )
```

```python
import functools
import math

import jax
import jax.numpy as jnp
from jax import lax
from jax.experimental import pallas as pl
from jax.experimental.pallas import tpu as pltpu
from jax.sharding import PartitionSpec as P

SWEEPS = 4
CUT = 32
PIECES = 4
HALF = math.sqrt(0.5)
MESH = pl.DeviceIdType.MESH


def to_modes(x):
    e = [x[n] + x[n + 4] for n in range(4)]
    o = [x[n] - x[n + 4] for n in range(4)]
    even, odd = e[0] + e[2], e[1] + e[3]
    minus, plus = HALF * (o[1] - o[3]), HALF * (o[1] + o[3])
    return [even + odd, even - odd, o[0] + minus, plus + o[2], e[0] - e[2], e[1] - e[3], o[0] - minus, plus - o[2]]


def from_modes(a):
    even, odd = 0.125 * (a[0] + a[1]), 0.125 * (a[0] - a[1])
    c2, s2 = 0.25 * a[4], 0.25 * a[5]
    e = [even + c2, odd + s2, even - c2, odd - s2]
    c, s = a[2] - a[6], a[3] + a[7]
    o = [0.25 * (a[2] + a[6]), (0.25 * HALF) * (s + c), 0.25 * (a[3] - a[7]), (0.25 * HALF) * (s - c)]
    return [e[n] + o[n] for n in range(4)] + [e[n] - o[n] for n in range(4)]


def kernel(cells, fs_hbm, forcing_hbm, diff_hbm, block_hbm, out,
           fs, forcing, diff, block, halo, local, fm, rm, neg, u, edge_out, edge_in, back, relay_fs, relay_u,
           load_sem, sent, halo_r, fs_r, part_r, x_r, y_r, back_r, relay_r):
    i, k = lax.axis_index("inst"), lax.axis_index("cells")
    peers = (i + 1 - 2 * lax.rem(i, 2), lax.rem(i + 2, 4), 3 - i)
    has_left, has_right = k > 0, k < cells - 1
    has_up, has_down = i > 0, i < 3
    direct_left, direct_right = has_left & (k != CUT), has_right & (k != CUT - 1)
    column, upper = lax.rem(k, CUT), k // CUT
    ways = (None, CUT - 1 - (CUT - 1) * (1 - upper), 7, 24)
    piece = sum(jnp.where(column == at, n, 0) for n, at in enumerate(ways) if n)
    relays = piece > 0
    own_rows = pl.ds(pl.multiple_of(8 * i, 8), 8)

    loads = [
        pltpu.make_async_copy(fs_hbm, fs, load_sem.at[0]),
        pltpu.make_async_copy(forcing_hbm, forcing, load_sem.at[1]),
        pltpu.make_async_copy(diff_hbm, diff, load_sem.at[2]),
        pltpu.make_async_copy(block_hbm, block, load_sem.at[3]),
        pltpu.make_async_copy(fs_hbm.at[:, :, :, own_rows, :], fm.at[pl.ds(2 * i, 2)], load_sem.at[4]),
    ]
    for load in loads:
        load.start()

    barrier = pltpu.get_barrier_semaphore()
    for peer in peers:
        pl.semaphore_signal(barrier, inc=1, device_id=(peer, k), device_id_type=MESH)

    def greet(target):
        pl.semaphore_signal(barrier, inc=1, device_id=(i, target), device_id_type=MESH)

    pl.when(direct_left)(lambda: greet(k - 1))
    pl.when(direct_right)(lambda: greet(k + 1))
    pl.when(relays)(lambda: greet(CUT - upper))

    @pl.when((k == CUT - 1) | (k == CUT))
    def _():
        for at in (upper * (2 * CUT - 1), upper * CUT + 7, upper * CUT + 24):
            greet(at)
        greet(CUT - upper)

    count = 3 + sum(jnp.where(held, n, 0) for held, n in (
        (direct_left, 1), (direct_right, 1), (relays, 1), ((k == CUT - 1) | (k == CUT), PIECES)))
    pl.semaphore_wait(barrier, count)

    def remote(src, dst, send, recv, device):
        return pltpu.make_async_remote_copy(
            src_ref=src, dst_ref=dst, send_sem=send, recv_sem=recv, device_id=device, device_id_type=MESH)

    def rows_of(peer):
        return pl.ds(pl.multiple_of(8 * peer, 8), 8)

    def fs_copy(x, slot):
        peer = peers[slot]
        return remote(fs.at[:, :, x, rows_of(peer), :], fm.at[pl.ds(2 * i, 2), :, x],
                      sent.at[0], fs_r.at[min(x, 7 - x)], (peer, k))

    def part_copy(x, slot):
        peer = peers[slot]
        return remote(local.at[:, :, x, rows_of(peer), :], rm.at[pl.ds(2 * i, 2), :, x],
                      sent.at[1], part_r.at[min(x, 7 - x)], (peer, k))

    def back_copy(x, slot):
        peer = peers[slot]
        return remote(back.at[peer, x], out.at[:, :, x, own_rows, :],
                      sent.at[2], back_r.at[min(x, 7 - x)], (peer, k))

    def pair(p):
        return (p, 7 - p)

    def send(copy, p):
        for slot in (1, 2, 0):
            for x in pair(p):
                copy(x, slot).start()

    def await_bytes(ref, sem):
        remote(ref, ref, sem, sem, (i, k)).wait_recv()

    six = fm.at[pl.ds(0, 6), :, pl.ds(0, 2)]

    pieces = range(PIECES)

    def fs_piece(ref, n, lead):
        return ref.at[n // 2, :, lead, pl.ds(16 * (n % 2), 16), :]

    def halo_piece(side, n):
        return halo.at[side, n // 2, :, pl.ds(16 * (n % 2), 16), :]

    def u_piece(s, x, n):
        return u.at[s, x, pl.ds(80 * n, 80), :]

    def fs_edge(side, n):
        return remote(fs_piece(fs, n, 7 if side else 0), halo_piece(1 - side, n),
                      sent.at[5 + side], halo_r.at[1 - side], (i, k + (1 if side else -1)))

    def x_edge(s, side, n):
        return remote(u_piece(s, 8 if side else 1, n), u_piece(s, 0 if side else 9, n),
                      sent.at[3 + side], x_r.at[s, 1 - side], (i, k + (1 if side else -1)))

    def way(side, n):
        return (i, (2 * CUT - 1, CUT + 7, CUT + 24)[n - 1] if side else (0, 7, 24)[n - 1])

    def fs_far(side, n):
        return remote(fs_piece(fs, n, 7 if side else 0), relay_fs, sent.at[5 + side], relay_r.at[SWEEPS], way(side, n))

    def x_far(s, side, n):
        return remote(u_piece(s, 8 if side else 1, n), relay_u.at[s], sent.at[3 + side], relay_r.at[s], way(side, n))

    def fs_relayed():
        target = halo.at[1 - upper, piece // 2, :, pl.ds(pl.multiple_of(16 * lax.rem(piece, 2), 16), 16), :]
        return remote(relay_fs, target, sent.at[10], halo_r.at[1 - upper], (i, CUT - 1 + upper))

    def x_relayed(s):
        target = u.at[s, 9 - 9 * upper, pl.ds(pl.multiple_of(80 * piece, 8), 80), :]
        return remote(relay_u.at[s], target, sent.at[9], x_r.at[s, 1 - upper], (i, CUT - 1 + upper))

    def send_edge(near, far, side):
        @pl.when(direct_right if side else direct_left)
        def _():
            for n in pieces:
                near(side, n).start()

        @pl.when(k == (CUT - 1 if side else CUT))
        def _():
            for n in pieces[1:]:
                far(side, n).start()
            near(side, 0).start()

    def relay(event, copy, buffer):
        @pl.when(relays)
        def _():
            await_bytes(buffer, relay_r.at[event])
            copy().start()

    def y_edge(s, p, side):
        return remote(edge_out.at[s, side, p], edge_in.at[s, 1 - side, p], sent.at[7 + side], y_r.at[s, 1 - side, p],
                      (i + (1 if side else -1), k))

    def both(first, second, action):
        pl.when(first)(lambda: action(0))
        pl.when(second)(lambda: action(1))

    loads[0].wait()
    for side in range(2):
        send_edge(fs_edge, fs_far, side)
    send(fs_copy, 0)
    send(fs_copy, 1)

    def clear(ref, lead):
        zeros = jnp.zeros((8, 128), jnp.float32)

        def body(t, carry):
            ref[(*lead, pl.ds(pl.multiple_of(8 * t, 8), 8), slice(None))] = zeros
            return carry

        lax.fori_loop(0, ref.shape[-2] // 8, body, 0)

    def clear_x(side):
        for n in range(2):
            for v in range(5):
                clear(halo, (side, n, v))
        for s in range(SWEEPS):
            clear(u, (s, 9 if side else 0))

    def clear_y(side):
        for s in range(SWEEPS):
            for p in range(4):
                for t in range(2):
                    clear(edge_in, (s, side, p, t))

    both(jnp.logical_not(has_left), jnp.logical_not(has_right), clear_x)
    both(jnp.logical_not(has_up), jnp.logical_not(has_down), clear_y)

    loads[1].wait()
    loads[2].wait()

    def shifted_sum(c, low, high):
        n = c.shape[0]
        row = lax.broadcasted_iota(jnp.int32, c.shape, 0)
        lane = lax.broadcasted_iota(jnp.int32, c.shape, 1)
        up = jnp.where(row == 0, low, pltpu.roll(c, 1, 0))
        down = jnp.where(row == n - 1, high, pltpu.roll(c, n - 1, 0))
        left = jnp.where(lane == 0, 0.0, pltpu.roll(c, 1, 1))
        right = jnp.where(lane == 127, 0.0, pltpu.roll(c, 127, 1))
        return (up + down) + (left + right)

    def local_plane(x, before, after):
        weight = diff[x]
        for n in range(2):
            for v in range(5):
                c = fs[n, v, x]
                beside = shifted_sum(c, 0.0, 0.0) + (before(n, v) + after(n, v))
                local[n, v, x] = weight * (6.0 * c - beside) - forcing[n, v, x]
        for n in range(2):
            for v in range(5):
                rm[2 * i + n, v, x] = local[n, v, x, own_rows, :]

    def inner(x, carry):
        local_plane(x, lambda n, v: fs[n, v, x - 1], lambda n, v: fs[n, v, x + 1])
        return carry

    lax.fori_loop(1, 7, inner, 0)

    send(part_copy, 1)
    relay(SWEEPS, fs_relayed, relay_fs)

    both(has_left, has_right, lambda side: await_bytes(halo.at[side], halo_r.at[side]))
    local_plane(0, lambda n, v: halo[0, n, v], lambda n, v: fs[n, v, 1])
    local_plane(7, lambda n, v: fs[n, v, 6], lambda n, v: halo[1, n, v])
    send(part_copy, 0)
    send(fs_copy, 2)
    loads[3].wait()
    loads[4].wait()

    def tile(m, v):
        return pl.ds((m * 5 + v) * 8, 8)

    def plane_of(p, t):
        return p + t * (7 - 2 * p)

    def store_edges(s, p, t, x):
        edge_out[s, 0, p, t] = u[s, x + 1, pl.ds(0, 40, stride=8), :]
        edge_out[s, 1, p, t] = u[s, x + 1, pl.ds(7, 40, stride=8), :]

    def apply_block(s, x, m, source):
        for v in range(5):
            total = block[v, 0, x] * source[0]
            for w in range(1, 5):
                total = total + block[v, w, x] * source[w]
            u[s, x + 1, tile(m, v), :] = total

    def first_plane(x):
        for v in range(5):
            f = to_modes([fm[n, v, x] for n in range(8)])
            r = to_modes([rm[n, v, x] for n in range(8)])
            neg[x, tile(0, v), :] = -r[0]
            neg[x, tile(1, v), :] = -r[1]
            for q in range(1, 4):
                neg[x, tile(2 * q, v), :] = -(r[2 * q] + q * f[2 * q + 1])
                neg[x, tile(2 * q + 1, v), :] = q * f[2 * q] - r[2 * q + 1]
        for m in range(8):
            apply_block(0, x, m, [neg[x, tile(m, v), :] for v in range(5)])

    def sweep_plane(s, p, t):
        x = plane_of(p, t)
        weight = diff[x, own_rows, :]
        for q in range(4):
            c = [[u[s - 1, x + 1, tile(2 * q + j, v), :] for v in range(5)] for j in range(2)]
            for j in range(2):
                source = []
                for v in range(5):
                    here = tile(2 * q + j, v)
                    at = (2 * q + j) * 5 + v
                    beside = shifted_sum(c[j][v], edge_in[s - 1, 0, p, t, pl.ds(at, 1), :],
                                         edge_in[s - 1, 1, p, t, pl.ds(at, 1), :])
                    beside = beside + (u[s - 1, x, here, :] + u[s - 1, x + 2, here, :])
                    value = weight * beside + neg[x, here, :]
                    if q:
                        value = value + (float(q) * c[0][v] if j else float(-q) * c[1][v])
                    source.append(value)
                apply_block(s, x, 2 * q + j, source)

    def back_plane(x):
        for v in range(5):
            modes = from_modes([u[SWEEPS, x + 1, tile(m, v), :] for m in range(8)])
            for n in range(8):
                back[n // 2, x, n % 2, v] = fm[n, v, x] + modes[n]
        for n in range(2):
            for v in range(5):
                out[n, v, x, own_rows, :] = back[i, x, n, v]

    def y_arrived(s, p):
        both(has_up, has_down, lambda side: await_bytes(edge_in.at[s, side, p], y_r.at[s, side, p]))

    def x_arrived(s):
        both(has_left, has_right, lambda side: await_bytes(u.at[s, 9 if side else 0], x_r.at[s, side]))

    def send_x(s, side):
        send_edge(functools.partial(x_edge, s), functools.partial(x_far, s), side)

    def run(s, p, body):
        def one(t, carry):
            body(t)
            if s < SWEEPS:
                store_edges(s, p, t, plane_of(p, t))
            return carry

        if p == 0 and s < SWEEPS:
            for t in range(2):
                one(t, 0)
                send_x(s, t)
        else:
            lax.fori_loop(0, 2, one, 0)
        if s < SWEEPS:
            both(has_up, has_down, lambda side: y_edge(s, p, side).start())

    for d in range(8):
        for p in ((0, 1), (), (2,), (3,), (), (), (), ())[d]:
            await_bytes(six, fs_r.at[p])
            await_bytes(six, part_r.at[p])
            run(0, p, lambda t: first_plane(plane_of(p, t)))
        if d == 0:
            send(part_copy, 2)
            send(fs_copy, 3)
        for s in range(max(1, d - 3), min(4, d) + 1):
            p = d - s
            y_arrived(s - 1, p)
            if p == 0:
                if s == SWEEPS:
                    relay(s - 1, functools.partial(x_relayed, s - 1), relay_u.at[s - 1])
                x_arrived(s - 1)

            def sweep(t):
                sweep_plane(s, p, t)
                if s == SWEEPS:
                    back_plane(plane_of(p, t))

            run(s, p, sweep)
            if s == SWEEPS:
                send(back_copy, p)
        if d == 1:
            send(part_copy, 3)
        if d < SWEEPS - 1:
            relay(d, functools.partial(x_relayed, d), relay_u.at[d])

    for p in range(4):
        await_bytes(six, back_r.at[p])

    def done(ref, sem):
        remote(ref, ref, sem, sem, (i, k)).wait_send()

    for n in range(3):
        done(fs.at[:, :, pl.ds(0, 6)], sent.at[n])

    def edges_done(side):
        done(u.at[pl.ds(0, SWEEPS), 1], sent.at[3 + side])
        done(halo.at[side], sent.at[5 + side])

    both(has_left, has_right, edges_done)
    both(has_up, has_down, lambda side: done(edge_out.at[:, side], sent.at[7 + side]))

    @pl.when(relays)
    def _():
        done(relay_u, sent.at[9])
        done(relay_fs, sent.at[10])


def store(source, target, sem):
    copies = [pltpu.make_async_copy(source.at[:, :, x], target.at[:, :, x], sem.at[x]) for x in range(8)]
    for copy in copies:
        copy.start()
    for copy in copies:
        copy.wait()


def on_device(cells, flow_state, forcing, diffusion, block_inverse):
    f32 = jnp.float32
    dma = pltpu.SemaphoreType.DMA
    any_spec = pl.BlockSpec(memory_space=pl.ANY)
    moved = pl.pallas_call(
        functools.partial(kernel, cells),
        out_shape=pltpu.VMEM(flow_state.shape, f32),
        in_specs=[any_spec] * 4,
        out_specs=pl.BlockSpec(memory_space=pltpu.VMEM),
        scratch_shapes=[
            pltpu.VMEM((2, 5, 8, 32, 128), f32),
            pltpu.VMEM((2, 5, 8, 32, 128), f32),
            pltpu.VMEM((8, 32, 128), f32),
            pltpu.VMEM((5, 5, 8, 8, 128), f32),
            pltpu.VMEM((2, 2, 5, 32, 128), f32),
            pltpu.VMEM((2, 5, 8, 32, 128), f32),
            pltpu.VMEM((8, 5, 8, 8, 128), f32),
            pltpu.VMEM((8, 5, 8, 8, 128), f32),
            pltpu.VMEM((8, 320, 128), f32),
            pltpu.VMEM((SWEEPS + 1, 10, 320, 128), f32),
            pltpu.VMEM((SWEEPS, 2, 4, 2, 40, 128), f32),
            pltpu.VMEM((SWEEPS, 2, 4, 2, 40, 128), f32),
            pltpu.VMEM((4, 8, 2, 5, 8, 128), f32),
            pltpu.VMEM((5, 16, 128), f32),
            pltpu.VMEM((SWEEPS, 80, 128), f32),
            dma((5,)),
            dma((11,)),
            dma((2,)), dma((4,)), dma((4,)), dma((SWEEPS, 2)), dma((SWEEPS, 2, 4)), dma((4,)), dma((SWEEPS + 1,)),
        ],
        compiler_params=pltpu.CompilerParams(
            collective_id=0, has_side_effects=True, vmem_limit_bytes=65640448),
        name="update",
    )(flow_state, forcing, diffusion, block_inverse)
    return pl.pallas_call(
        store, out_shape=jax.ShapeDtypeStruct(flow_state.shape, f32), in_specs=[any_spec], out_specs=any_spec,
        scratch_shapes=[dma((8,))], compiler_params=pltpu.CompilerParams(vmem_limit_bytes=8 * 1024 * 1024), name="store",
    )(moved)


def solution(mesh):
    in_specs = (
        P("inst", None, "cells", None, None),
        P("inst", None, "cells", None, None),
        P("cells", None, None),
        P(None, None, "cells", "inst", None),
    )
    out_specs = P("inst", None, "cells", None, None)
    return jax.shard_map(
        functools.partial(on_device, mesh.shape["cells"]),
        mesh=mesh, in_specs=in_specs, out_specs=out_specs, check_vma=False,
    )
```

```python
import functools
import math

import jax
import jax.numpy as jnp
from jax import lax
from jax.experimental import pallas as pl
from jax.experimental.pallas import tpu as pltpu
from jax.sharding import PartitionSpec as P

SWEEPS = 4
CUT = 32
PIECES = 4
RELAYED = 2
HALF = math.sqrt(0.5)
MESH = pl.DeviceIdType.MESH


def to_modes(x):
    e = [x[n] + x[n + 4] for n in range(4)]
    o = [x[n] - x[n + 4] for n in range(4)]
    even, odd = e[0] + e[2], e[1] + e[3]
    minus, plus = HALF * (o[1] - o[3]), HALF * (o[1] + o[3])
    return [even + odd, even - odd, o[0] + minus, plus + o[2], e[0] - e[2], e[1] - e[3], o[0] - minus, plus - o[2]]


def from_modes(a):
    even, odd = 0.125 * (a[0] + a[1]), 0.125 * (a[0] - a[1])
    c2, s2 = 0.25 * a[4], 0.25 * a[5]
    e = [even + c2, odd + s2, even - c2, odd - s2]
    c, s = a[2] - a[6], a[3] + a[7]
    o = [0.25 * (a[2] + a[6]), (0.25 * HALF) * (s + c), 0.25 * (a[3] - a[7]), (0.25 * HALF) * (s - c)]
    return [e[n] + o[n] for n in range(4)] + [e[n] - o[n] for n in range(4)]


def kernel(cells, fs_hbm, forcing_hbm, diff_hbm, block_hbm, out,
           fs, forcing, diff, block, halo, local, fm, rm, neg, u, edge_out, edge_in, back, relay_fs, relay_u,
           load_sem, sent, halo_r, fs_r, part_r, x_r, y_r, back_r, relay_r):
    i, k = lax.axis_index("inst"), lax.axis_index("cells")
    peers = (i + 1 - 2 * lax.rem(i, 2), lax.rem(i + 2, 4), 3 - i)
    has_left, has_right = k > 0, k < cells - 1
    has_up, has_down = i > 0, i < 3
    direct_left, direct_right = has_left & (k != CUT), has_right & (k != CUT - 1)
    column, upper = lax.rem(k, CUT), k // CUT
    ways = (None, None, 7, 24)
    piece = sum(jnp.where(column == at, n, 0) for n, at in enumerate(ways) if at)
    relays = piece > 0
    own_rows = pl.ds(pl.multiple_of(8 * i, 8), 8)

    loads = [
        pltpu.make_async_copy(fs_hbm, fs, load_sem.at[0]),
        pltpu.make_async_copy(forcing_hbm, forcing, load_sem.at[1]),
        pltpu.make_async_copy(diff_hbm, diff, load_sem.at[2]),
        pltpu.make_async_copy(block_hbm, block, load_sem.at[3]),
        pltpu.make_async_copy(fs_hbm.at[:, :, :, own_rows, :], fm.at[pl.ds(2 * i, 2)], load_sem.at[4]),
    ]
    for load in loads:
        load.start()

    barrier = pltpu.get_barrier_semaphore()
    for peer in peers:
        pl.semaphore_signal(barrier, inc=1, device_id=(peer, k), device_id_type=MESH)

    def greet(target):
        pl.semaphore_signal(barrier, inc=1, device_id=(i, target), device_id_type=MESH)

    pl.when(direct_left)(lambda: greet(k - 1))
    pl.when(direct_right)(lambda: greet(k + 1))
    pl.when(relays)(lambda: greet(CUT - upper))

    @pl.when((k == CUT - 1) | (k == CUT))
    def _():
        for at in ways:
            if at is not None:
                greet(upper * CUT + at)
        greet(CUT - upper)

    count = 3 + sum(jnp.where(held, n, 0) for held, n in (
        (direct_left, 1), (direct_right, 1), (relays, 1), ((k == CUT - 1) | (k == CUT), 1 + sum(at is not None for at in ways))))
    pl.semaphore_wait(barrier, count)

    def remote(src, dst, send, recv, device):
        return pltpu.make_async_remote_copy(
            src_ref=src, dst_ref=dst, send_sem=send, recv_sem=recv, device_id=device, device_id_type=MESH)

    def rows_of(peer):
        return pl.ds(pl.multiple_of(8 * peer, 8), 8)

    def fs_copy(x, slot):
        peer = peers[slot]
        return remote(fs.at[:, :, x, rows_of(peer), :], fm.at[pl.ds(2 * i, 2), :, x],
                      sent.at[0], fs_r.at[min(x, 7 - x)], (peer, k))

    def part_copy(x, slot):
        peer = peers[slot]
        return remote(local.at[:, :, x, rows_of(peer), :], rm.at[pl.ds(2 * i, 2), :, x],
                      sent.at[1], part_r.at[min(x, 7 - x)], (peer, k))

    def back_copy(x, slot):
        peer = peers[slot]
        return remote(back.at[peer, x], out.at[:, :, x, own_rows, :],
                      sent.at[2], back_r.at[min(x, 7 - x)], (peer, k))

    def pair(p):
        return (p, 7 - p)

    def send(copy, p):
        for slot in (1, 2, 0):
            for x in pair(p):
                copy(x, slot).start()

    def await_bytes(ref, sem):
        remote(ref, ref, sem, sem, (i, k)).wait_recv()

    six = fm.at[pl.ds(0, 6), :, pl.ds(0, 2)]

    pieces = range(PIECES)

    def fs_piece(ref, n, lead):
        return ref.at[n // 2, :, lead, pl.ds(16 * (n % 2), 16), :]

    def halo_piece(side, n):
        return halo.at[side, n // 2, :, pl.ds(16 * (n % 2), 16), :]

    def u_piece(s, x, n):
        return u.at[s, x, pl.ds(80 * n, 80), :]

    def fs_edge(side, n):
        return remote(fs_piece(fs, n, 7 if side else 0), halo_piece(1 - side, n),
                      sent.at[5 + side], halo_r.at[1 - side], (i, k + (1 if side else -1)))

    def x_edge(s, side, n):
        return remote(u_piece(s, 8 if side else 1, n), u_piece(s, 0 if side else 9, n),
                      sent.at[3 + side], x_r.at[s, 1 - side], (i, k + (1 if side else -1)))

    def way(side, n):
        return (i, CUT * side + ways[n])

    def fs_far(side, n):
        return remote(fs_piece(fs, n, 7 if side else 0), relay_fs, sent.at[5 + side], relay_r.at[SWEEPS], way(side, n))

    def x_far(s, side, n):
        return remote(u_piece(s, 8 if side else 1, n), relay_u.at[s], sent.at[3 + side], relay_r.at[s], way(side, n))

    def fs_relayed():
        target = halo.at[1 - upper, piece // 2, :, pl.ds(pl.multiple_of(16 * lax.rem(piece, 2), 16), 16), :]
        return remote(relay_fs, target, sent.at[10], halo_r.at[1 - upper], (i, CUT - 1 + upper))

    def x_relayed(s):
        target = u.at[s, 9 - 9 * upper, pl.ds(pl.multiple_of(80 * piece, 8), 80), :]
        return remote(relay_u.at[s], target, sent.at[9], x_r.at[s, 1 - upper], (i, CUT - 1 + upper))

    def send_edge(near, far, side):
        @pl.when(direct_right if side else direct_left)
        def _():
            for n in pieces:
                near(side, n).start()

        @pl.when(k == (CUT - 1 if side else CUT))
        def _():
            for n in pieces:
                (near if ways[n] is None else far)(side, n).start()

    def relay(event, copy, buffer):
        @pl.when(relays)
        def _():
            await_bytes(buffer, relay_r.at[event])
            copy().start()

    def y_edge(s, p, side):
        return remote(edge_out.at[s, side, p], edge_in.at[s, 1 - side, p], sent.at[7 + side], y_r.at[s, 1 - side, p],
                      (i + (1 if side else -1), k))

    def both(first, second, action):
        pl.when(first)(lambda: action(0))
        pl.when(second)(lambda: action(1))

    loads[0].wait()
    for side in range(2):
        send_edge(fs_edge, fs_far, side)
    send(fs_copy, 0)
    send(fs_copy, 1)

    def clear(ref, lead):
        zeros = jnp.zeros((8, 128), jnp.float32)

        def body(t, carry):
            ref[(*lead, pl.ds(pl.multiple_of(8 * t, 8), 8), slice(None))] = zeros
            return carry

        lax.fori_loop(0, ref.shape[-2] // 8, body, 0)

    def clear_x(side):
        for n in range(2):
            for v in range(5):
                clear(halo, (side, n, v))
        for s in range(SWEEPS):
            clear(u, (s, 9 if side else 0))

    def clear_y(side):
        for s in range(SWEEPS):
            for p in range(4):
                for t in range(2):
                    clear(edge_in, (s, side, p, t))

    both(jnp.logical_not(has_left), jnp.logical_not(has_right), clear_x)
    both(jnp.logical_not(has_up), jnp.logical_not(has_down), clear_y)

    loads[1].wait()
    loads[2].wait()

    def shifted_sum(c, low, high):
        n = c.shape[0]
        row = lax.broadcasted_iota(jnp.int32, c.shape, 0)
        lane = lax.broadcasted_iota(jnp.int32, c.shape, 1)
        up = jnp.where(row == 0, low, pltpu.roll(c, 1, 0))
        down = jnp.where(row == n - 1, high, pltpu.roll(c, n - 1, 0))
        left = jnp.where(lane == 0, 0.0, pltpu.roll(c, 1, 1))
        right = jnp.where(lane == 127, 0.0, pltpu.roll(c, 127, 1))
        return (up + down) + (left + right)

    def local_plane(x, before, after):
        weight = diff[x]
        for n in range(2):
            for v in range(5):
                c = fs[n, v, x]
                beside = shifted_sum(c, 0.0, 0.0) + (before(n, v) + after(n, v))
                local[n, v, x] = weight * (6.0 * c - beside) - forcing[n, v, x]
        for n in range(2):
            for v in range(5):
                rm[2 * i + n, v, x] = local[n, v, x, own_rows, :]

    def inner(x, carry):
        local_plane(x, lambda n, v: fs[n, v, x - 1], lambda n, v: fs[n, v, x + 1])
        return carry

    lax.fori_loop(1, 7, inner, 0)

    relay(SWEEPS, fs_relayed, relay_fs)

    both(has_left, has_right, lambda side: await_bytes(halo.at[side], halo_r.at[side]))
    local_plane(0, lambda n, v: halo[0, n, v], lambda n, v: fs[n, v, 1])
    local_plane(7, lambda n, v: fs[n, v, 6], lambda n, v: halo[1, n, v])
    send(part_copy, 0)
    send(part_copy, 1)
    send(fs_copy, 2)
    loads[3].wait()
    loads[4].wait()

    def tile(m, v):
        return pl.ds((m * 5 + v) * 8, 8)

    def plane_of(p, t):
        return p + t * (7 - 2 * p)

    def store_edges(s, p, t, x):
        edge_out[s, 0, p, t] = u[s, x + 1, pl.ds(0, 40, stride=8), :]
        edge_out[s, 1, p, t] = u[s, x + 1, pl.ds(7, 40, stride=8), :]

    def apply_block(s, x, m, source):
        for v in range(5):
            total = block[v, 0, x] * source[0]
            for w in range(1, 5):
                total = total + block[v, w, x] * source[w]
            u[s, x + 1, tile(m, v), :] = total

    def first_plane(x):
        for v in range(5):
            f = to_modes([fm[n, v, x] for n in range(8)])
            r = to_modes([rm[n, v, x] for n in range(8)])
            neg[x, tile(0, v), :] = -r[0]
            neg[x, tile(1, v), :] = -r[1]
            for q in range(1, 4):
                neg[x, tile(2 * q, v), :] = -(r[2 * q] + q * f[2 * q + 1])
                neg[x, tile(2 * q + 1, v), :] = q * f[2 * q] - r[2 * q + 1]
        for m in range(8):
            apply_block(0, x, m, [neg[x, tile(m, v), :] for v in range(5)])

    def sweep_plane(s, p, t):
        x = plane_of(p, t)
        weight = diff[x, own_rows, :]
        for q in range(4):
            c = [[u[s - 1, x + 1, tile(2 * q + j, v), :] for v in range(5)] for j in range(2)]
            for j in range(2):
                source = []
                for v in range(5):
                    here = tile(2 * q + j, v)
                    at = (2 * q + j) * 5 + v
                    beside = shifted_sum(c[j][v], edge_in[s - 1, 0, p, t, pl.ds(at, 1), :],
                                         edge_in[s - 1, 1, p, t, pl.ds(at, 1), :])
                    beside = beside + (u[s - 1, x, here, :] + u[s - 1, x + 2, here, :])
                    value = weight * beside + neg[x, here, :]
                    if q:
                        value = value + (float(q) * c[0][v] if j else float(-q) * c[1][v])
                    source.append(value)
                apply_block(s, x, 2 * q + j, source)

    def back_plane(x):
        for v in range(5):
            modes = from_modes([u[SWEEPS, x + 1, tile(m, v), :] for m in range(8)])
            for n in range(8):
                back[n // 2, x, n % 2, v] = fm[n, v, x] + modes[n]
        for n in range(2):
            for v in range(5):
                out[n, v, x, own_rows, :] = back[i, x, n, v]

    def y_arrived(s, p):
        both(has_up, has_down, lambda side: await_bytes(edge_in.at[s, side, p], y_r.at[s, side, p]))

    def x_arrived(s):
        both(has_left, has_right, lambda side: await_bytes(u.at[s, 9 if side else 0], x_r.at[s, side]))

    def send_x(s, side):
        near = functools.partial(x_edge, s)
        send_edge(near, functools.partial(x_far, s) if s < RELAYED else near, side)

    def run(s, p, body):
        def one(t, carry):
            body(t)
            if s < SWEEPS:
                store_edges(s, p, t, plane_of(p, t))
            return carry

        if p == 0 and s < SWEEPS:
            for t in range(2):
                one(t, 0)
                send_x(s, t)
        else:
            lax.fori_loop(0, 2, one, 0)
        if s < SWEEPS:
            both(has_up, has_down, lambda side: y_edge(s, p, side).start())

    for d in range(8):
        for p in ((0, 1), (), (2,), (3,), (), (), (), ())[d]:
            await_bytes(six, fs_r.at[p])
            await_bytes(six, part_r.at[p])
            run(0, p, lambda t: first_plane(plane_of(p, t)))
        if d == 0:
            send(part_copy, 2)
            send(fs_copy, 3)
        for s in range(max(1, d - 3), min(4, d) + 1):
            p = d - s
            y_arrived(s - 1, p)
            if p == 0:
                x_arrived(s - 1)

            def sweep(t):
                sweep_plane(s, p, t)
                if s == SWEEPS:
                    back_plane(plane_of(p, t))

            run(s, p, sweep)
            if s == SWEEPS:
                send(back_copy, p)
        if d == 1:
            send(part_copy, 3)
        if d < RELAYED:
            relay(d, functools.partial(x_relayed, d), relay_u.at[d])

    for p in range(4):
        await_bytes(six, back_r.at[p])

    def done(ref, sem):
        remote(ref, ref, sem, sem, (i, k)).wait_send()

    for n in range(3):
        done(fs.at[:, :, pl.ds(0, 6)], sent.at[n])

    def edges_done(side):
        done(u.at[pl.ds(0, SWEEPS), 1], sent.at[3 + side])
        done(halo.at[side], sent.at[5 + side])

    both(has_left, has_right, edges_done)
    both(has_up, has_down, lambda side: done(edge_out.at[:, side], sent.at[7 + side]))

    @pl.when(relays)
    def _():
        done(relay_u.at[pl.ds(0, RELAYED)], sent.at[9])
        done(relay_fs, sent.at[10])


def store(source, target, sem):
    copies = [pltpu.make_async_copy(source.at[:, :, x], target.at[:, :, x], sem.at[x]) for x in range(8)]
    for copy in copies:
        copy.start()
    for copy in copies:
        copy.wait()


def on_device(cells, flow_state, forcing, diffusion, block_inverse):
    f32 = jnp.float32
    dma = pltpu.SemaphoreType.DMA
    any_spec = pl.BlockSpec(memory_space=pl.ANY)
    moved = pl.pallas_call(
        functools.partial(kernel, cells),
        out_shape=pltpu.VMEM(flow_state.shape, f32),
        in_specs=[any_spec] * 4,
        out_specs=pl.BlockSpec(memory_space=pltpu.VMEM),
        scratch_shapes=[
            pltpu.VMEM((2, 5, 8, 32, 128), f32),
            pltpu.VMEM((2, 5, 8, 32, 128), f32),
            pltpu.VMEM((8, 32, 128), f32),
            pltpu.VMEM((5, 5, 8, 8, 128), f32),
            pltpu.VMEM((2, 2, 5, 32, 128), f32),
            pltpu.VMEM((2, 5, 8, 32, 128), f32),
            pltpu.VMEM((8, 5, 8, 8, 128), f32),
            pltpu.VMEM((8, 5, 8, 8, 128), f32),
            pltpu.VMEM((8, 320, 128), f32),
            pltpu.VMEM((SWEEPS + 1, 10, 320, 128), f32),
            pltpu.VMEM((SWEEPS, 2, 4, 2, 40, 128), f32),
            pltpu.VMEM((SWEEPS, 2, 4, 2, 40, 128), f32),
            pltpu.VMEM((4, 8, 2, 5, 8, 128), f32),
            pltpu.VMEM((5, 16, 128), f32),
            pltpu.VMEM((SWEEPS, 80, 128), f32),
            dma((5,)),
            dma((11,)),
            dma((2,)), dma((4,)), dma((4,)), dma((SWEEPS, 2)), dma((SWEEPS, 2, 4)), dma((4,)), dma((SWEEPS + 1,)),
        ],
        compiler_params=pltpu.CompilerParams(
            collective_id=0, has_side_effects=True, vmem_limit_bytes=65640448),
        name="update",
    )(flow_state, forcing, diffusion, block_inverse)
    return pl.pallas_call(
        store, out_shape=jax.ShapeDtypeStruct(flow_state.shape, f32), in_specs=[any_spec], out_specs=any_spec,
        scratch_shapes=[dma((8,))], compiler_params=pltpu.CompilerParams(vmem_limit_bytes=8 * 1024 * 1024), name="store",
    )(moved)


def solution(mesh):
    in_specs = (
        P("inst", None, "cells", None, None),
        P("inst", None, "cells", None, None),
        P("cells", None, None),
        P(None, None, "cells", "inst", None),
    )
    out_specs = P("inst", None, "cells", None, None)
    return jax.shard_map(
        functools.partial(on_device, mesh.shape["cells"]),
        mesh=mesh, in_specs=in_specs, out_specs=out_specs, check_vma=False,
    )
```
